32 devices in a mesh: clip: 4 (over y, core), seq: 8 (over z, x).
Axes of the slice: x: 2, y: 2, z: 4, core: 2. Of those that a mesh axis runs over, the one named last changes fastest.
Arguments:
- block_input: bfloat16 [64, 384, 1152], P('clip', 'seq'), parts along dimension 0, may hold values from -160 to 160
- mid_state: bfloat16 [64, 384, 1152], P('clip', 'seq'), parts along dimension 0, may hold values from -160 to 160
- saved_qkv: bfloat16 [3, 64, 384, 576], P(None, 'clip', 'seq'), parts along dimension 1, may hold values from -6 to 6
- out_grad: bfloat16 [64, 384, 1152], P('clip', 'seq'), parts along dimension 0, may hold values from -6 to 6
- modulation: float32 [20, 1152], P('clip'), parts along dimension 0, may hold values from -3 to 3
- w_qkv_s: bfloat16 [1152, 1728], replicated, may hold values from -0.1875 to 0.1875
- w_out_s: bfloat16 [576, 1152], replicated, may hold values from -0.25 to 0.25
- w_qkv_t: bfloat16 [1152, 1728], replicated, may hold values from -0.1875 to 0.1875
- w_out_t: bfloat16 [576, 1152], replicated, may hold values from -0.25 to 0.25
- qk_gain: float32 [4, 72], replicated, may hold values from 0.1 to 1.9
Outputs:
- input_grad: bfloat16 [64, 384, 1152], P('clip', 'seq'), parts along dimension 0
- mod_grad: float32 [24, 1152], P('clip'), parts along dimension 0
The draws below stay inside these ranges and needn't reach their ends.
There are 4 independent parts, one for each index of `clip`. The reference program is written for one: setup_inputs(seed, part) draws one part's arguments, and reference() takes and returns one part's arrays. A program takes and returns all parts, laid end to end along the dimension named above; an argument that names none is the same for every part. Nothing has to cross between parts.
All inputs are finite; a program needn't handle non-finite values.
Results may differ from the reference program's by a relative error of at most 0.0057.
Values may be sent and summed in bfloat16 or wider, within the bound.
No kernel may reach another device: no remote copies, remote signals or barrier semaphores. Data moves between devices by JAX's collectives and lax.ppermute only.
A program may use at most 128 MiB of HBM per device.

```python
import math
import jax
import jax.numpy as jnp
from jax import lax

D = 1152
HEADS = 8
HEAD_DIM = 72
WIDTH = 576
SPATIAL = 384
FRAMES = 16
TOKENS = 6144


def feature_draw(key, salt):
    salted = jax.random.fold_in(key, salt)
    subkeys = jax.random.split(salted, 3)
    full_shape = (FRAMES, SPATIAL, D)
    col_scale = jnp.exp(jax.random.uniform(subkeys[0], (D,), jnp.float32, 0.0, math.log(10.0)))
    row_scale = jnp.exp(jax.random.uniform(subkeys[1], (FRAMES, SPATIAL, 1), jnp.float32, 0.0, math.log(4.0)))
    drawn = jnp.clip(jax.random.normal(subkeys[2], full_shape, jnp.float32), -3.9, 3.9)
    return (drawn * row_scale * col_scale).astype(jnp.bfloat16)


def draw_block_input(key, part):
    return feature_draw(key, 11)


def draw_mid_state(key, part):
    return feature_draw(key, 23)


def shard_levels(stream_key, extent, shards, low, largest):
    def one(dim, shards_of):
        steps = jax.random.uniform(jax.random.fold_in(jax.random.fold_in(stream_key, 6), dim), (shards_of,), jnp.float32, low / len(shards), largest / len(shards))
        return jnp.repeat(jnp.exp(steps), extent[dim] // shards_of).reshape((-1,) + (1,) * (len(extent) - dim - 1))

    loudness = one(*shards[0])
    for cut in shards[1:]:
        loudness = loudness * one(*cut)
    return loudness


def normal_values(own_key, extent, deviation, limit, cuts=(), dtype=jnp.bfloat16):
    values = jax.random.normal(own_key, extent, jnp.float32) * deviation
    if len(cuts) > 0:
        values = shard_levels(own_key, extent, cuts, -0.22, 0.18) * values
    return jnp.clip(values, min=-limit, max=limit).astype(dtype)


def setup_inputs(seed: int = 0, part: int = 0) -> dict:
    keys = jax.random.split(jax.random.key(seed), 11)
    part_keys = jax.random.split(jax.random.fold_in(keys[10], part), 11)
    block_input = draw_block_input(jax.random.fold_in(jax.random.fold_in(keys[10], part), 71), part)
    mid_state = draw_mid_state(jax.random.fold_in(jax.random.fold_in(keys[10], part), 71), part)
    saved_qkv = normal_values(part_keys[2], (3, FRAMES, SPATIAL, WIDTH), 1.0, 6.0, ((2, 8),))
    out_grad = normal_values(part_keys[3], (FRAMES, SPATIAL, D), 1.0, 6.0, ((1, 8),))
    modulation = normal_values(part_keys[4], (5, D), 0.5, 3.0, (), jnp.float32)
    w_qkv_s = normal_values(keys[5], (D, 3 * WIDTH), D ** -0.5, 0.1875)
    w_out_s = normal_values(keys[6], (WIDTH, D), WIDTH ** -0.5, 0.25)
    w_qkv_t = normal_values(keys[7], (D, 3 * WIDTH), D ** -0.5, 0.1875)
    w_out_t = normal_values(keys[8], (WIDTH, D), WIDTH ** -0.5, 0.25)
    qk_gain = jnp.clip(1.0 + 0.18 * jax.random.normal(keys[9], (4, HEAD_DIM), jnp.float32), 0.1, 1.9)
    return dict(block_input=block_input, mid_state=mid_state, saved_qkv=saved_qkv, out_grad=out_grad, modulation=modulation, w_qkv_s=w_qkv_s, w_out_s=w_out_s, w_qkv_t=w_qkv_t, w_out_t=w_out_t, qk_gain=qk_gain)


NORM_EPS = 1e-06

def layer_stats(inputs):
    values = inputs.astype(jnp.float32)
    centre = lax.optimization_barrier(jnp.mean(values, axis=-1, keepdims=True))
    spread = lax.optimization_barrier(jnp.mean(jnp.square(values - centre), axis=-1, keepdims=True))
    inverse = lax.rsqrt(spread + NORM_EPS)
    return ((values - centre) * inverse, inverse)

def modulate(normed, offset, stretch):
    return (normed * (1.0 + stretch) + offset).astype(jnp.bfloat16)

def matmul_rows(left_rows, weight):
    flattened = left_rows.reshape(-1, left_rows.shape[-1])
    result = jnp.dot(flattened, weight, preferred_element_type=jnp.float32)
    return result.reshape(left_rows.shape[:-1] + (weight.shape[1],))

def matmul_back(left_rows, weight):
    flattened = left_rows.reshape(-1, left_rows.shape[-1])
    result = jnp.dot(flattened, weight.T, preferred_element_type=jnp.float32)
    return result.reshape(left_rows.shape[:-1] + (weight.shape[0],))

def head_split(tensor):
    return tensor.reshape(tensor.shape[:-1] + (HEADS, HEAD_DIM))

def rms_normed(raw_rows, gain_row):
    values = head_split(raw_rows).astype(jnp.float32)
    inverse = lax.rsqrt(lax.optimization_barrier(jnp.mean(values * values, axis=-1, keepdims=True)) + NORM_EPS)
    return ((values * inverse * gain_row).astype(jnp.bfloat16), values, inverse)

def rms_back(values, inverse, gain_row, upstream):
    scaled = gain_row * upstream
    result = inverse * scaled - values * (inverse * inverse * inverse) * lax.optimization_barrier(jnp.mean(values * scaled, axis=-1, keepdims=True))
    return result.astype(jnp.bfloat16).reshape(values.shape[:-2] + (-1,))

def attend(queries, key_rows, value_rows, out_cot, query_gain, key_gain):
    query_norm, query_raw, query_inv = rms_normed(queries, query_gain)
    key_norm, key_raw, key_inv = rms_normed(key_rows, key_gain)
    factor = HEAD_DIM ** (-0.5)
    scores = jnp.einsum('blhd,bmhd->bhlm', query_norm.astype(jnp.float32), key_norm.astype(jnp.float32)) * factor
    exp_scores = jnp.exp(scores)
    attn_probs = exp_scores / lax.optimization_barrier(jnp.sum(exp_scores, axis=-1, keepdims=True))
    probs_half = attn_probs.astype(jnp.bfloat16)
    value_heads = head_split(value_rows).astype(jnp.float32)
    cot_heads = head_split(out_cot).astype(jnp.float32)
    outputs = jnp.einsum('bhlm,bmhd->blhd', probs_half.astype(jnp.float32), value_heads).astype(jnp.bfloat16)
    prob_grad = jnp.einsum('blhd,bmhd->bhlm', cot_heads, value_heads)
    row_inner = lax.optimization_barrier(jnp.sum(attn_probs * prob_grad, axis=-1, keepdims=True))
    score_grad = (attn_probs * (prob_grad - row_inner) * factor).astype(jnp.bfloat16).astype(jnp.float32)
    value_grad = jnp.einsum('bhlm,blhd->bmhd', probs_half.astype(jnp.float32), cot_heads).astype(jnp.bfloat16)
    qnorm_grad = jnp.einsum('bhlm,bmhd->blhd', score_grad, key_norm.astype(jnp.float32))
    knorm_grad = jnp.einsum('bhlm,blhd->bmhd', score_grad, query_norm.astype(jnp.float32))
    merged = outputs.shape[:-2] + (-1,)
    return (outputs.reshape(merged), rms_back(query_raw, query_inv, query_gain, qnorm_grad), rms_back(key_raw, key_inv, key_gain, knorm_grad), value_grad.reshape(merged))

def output_cot(cotangent, gate_row, w_out):
    scaled = (cotangent.astype(jnp.float32) * gate_row).astype(jnp.bfloat16)
    return matmul_back(scaled, w_out).astype(jnp.bfloat16)

def gate_term(cotangent, outputs, w_out):
    branch = matmul_rows(outputs, w_out)
    return lax.optimization_barrier(jnp.sum((cotangent.astype(jnp.float32) * branch).reshape(-1, branch.shape[-1]), axis=0))

def input_branch(grad_parts, w_qkv, normed, inverse, stretch):
    joined = jnp.concatenate(grad_parts, axis=-1)
    mod_cot = matmul_back(joined, w_qkv)
    columns = mod_cot.shape[-1]
    offset_term = lax.optimization_barrier(jnp.sum(mod_cot.reshape(-1, columns), axis=0))
    stretch_term = lax.optimization_barrier(jnp.sum((mod_cot * normed).reshape(-1, columns), axis=0))
    norm_cot = mod_cot * (1.0 + stretch)
    branch = inverse * (norm_cot - lax.optimization_barrier(jnp.mean(norm_cot, axis=-1, keepdims=True)) - normed * lax.optimization_barrier(jnp.mean(norm_cot * normed, axis=-1, keepdims=True)))
    return (branch, offset_term, stretch_term)

def swapped(tensor):
    return jnp.swapaxes(tensor, 0, 1)

def reference(block_input, mid_state, saved_qkv, out_grad, modulation, w_qkv_s, w_out_s, w_qkv_t, w_out_t, qk_gain):
    normed_mid, inverse_mid = layer_stats(mid_state)
    temporal_cot = output_cot(out_grad, modulation[4], w_out_t)
    temporal_res = attend(swapped(saved_qkv[0]), swapped(saved_qkv[1]), swapped(saved_qkv[2]), swapped(temporal_cot), qk_gain[2], qk_gain[3])
    temporal_gate = gate_term(out_grad, swapped(temporal_res[0]), w_out_t)
    temporal_branch, temporal_offset, temporal_stretch = input_branch(tuple((swapped(grad_piece) for grad_piece in temporal_res[1:])), w_qkv_t, normed_mid, inverse_mid, modulation[3])
    mid_grad = (out_grad.astype(jnp.float32) + temporal_branch).astype(jnp.bfloat16)

    def one_frame(frame_args):
        frame_in, frame_grad = frame_args
        normed_fr, inverse_fr = layer_stats(frame_in)
        frame_mod = modulate(normed_fr, modulation[0], modulation[1])
        frame_qkv = matmul_rows(frame_mod, w_qkv_s).astype(jnp.bfloat16)
        frame_cot = output_cot(frame_grad, modulation[2], w_out_s)
        frame_res = attend(frame_qkv[None, :, :WIDTH], frame_qkv[None, :, WIDTH:2 * WIDTH], frame_qkv[None, :, 2 * WIDTH:], frame_cot[None], qk_gain[0], qk_gain[1])
        gate_part = gate_term(frame_grad, frame_res[0][0], w_out_s)
        branch, offset_part, stretch_part = input_branch(tuple((grad_piece[0] for grad_piece in frame_res[1:])), w_qkv_s, normed_fr, inverse_fr, modulation[1])
        return (branch.astype(jnp.bfloat16), jnp.stack([offset_part, stretch_part, gate_part]))
    spatial_branch, frame_terms = lax.map(one_frame, (block_input, mid_grad))
    spatial_sums = lax.optimization_barrier(jnp.sum(frame_terms, axis=0))
    term_stack = jnp.concatenate([spatial_sums, jnp.stack([temporal_offset, temporal_stretch, temporal_gate])], axis=0)
    mod_grad = term_stack * TOKENS ** (-0.5)
    input_grad = (mid_grad.astype(jnp.float32) + spatial_branch.astype(jnp.float32)).astype(jnp.bfloat16)
    return (input_grad, mod_grad)
```

```python
import functools
import math

import jax
import jax.numpy as jnp
from jax import lax
from jax.experimental import pallas as pl
from jax.experimental.pallas import tpu as pltpu
from jax.sharding import PartitionSpec as P

HEAD_DIM = 72
NORM_EPS = 1e-06
LANES = 128
GROUP = 8
F32 = jnp.float32
BF16 = jnp.bfloat16


def nt(a, b):
    return lax.dot_general(a, b, (((1,), (1,)), ((), ())), preferred_element_type=F32)


def nn(a, b):
    return lax.dot_general(a, b, (((1,), (0,)), ((), ())), preferred_element_type=F32)


def tn(a, b):
    return lax.dot_general(a, b, (((0,), (0,)), ((), ())), preferred_element_type=F32)


def windows(width):
    pairs = width // (2 * HEAD_DIM)
    return [(LANES * p, min(2 * LANES, width - LANES * p), 2 * HEAD_DIM * p - LANES * p) for p in range(pairs)]


def attention_pair(q, k, v, c, gain_q, gain_k, first, same):
    rows, lanes = q.shape
    lane = lax.broadcasted_iota(jnp.int32, (1, lanes), 1)
    in0 = jnp.logical_and(lane >= first, lane < first + HEAD_DIM)
    in1 = jnp.logical_and(lane >= first + HEAD_DIM, lane < first + 2 * HEAD_DIM)
    m0, m1 = in0.astype(F32), in1.astype(F32)
    b0, b1 = m0.astype(BF16), m1.astype(BF16)

    def head_mean(t):
        mean0 = jnp.sum(t * m0, axis=-1, keepdims=True) * (1.0 / HEAD_DIM)
        mean1 = jnp.sum(t * m1, axis=-1, keepdims=True) * (1.0 / HEAD_DIM)
        return mean0, mean1

    def norm(t):
        mean0, mean1 = head_mean(t * t)
        return lax.rsqrt(mean0 + NORM_EPS) * m0 + lax.rsqrt(mean1 + NORM_EPS) * m1

    def both(t):
        return jnp.concatenate([t * b0, t * b1], axis=0)

    def stacked(t):
        return jnp.concatenate([t[:, :rows], t[:, rows:]], axis=0)

    rq, rk = norm(q), norm(k)
    qn = (q * rq * gain_q).astype(BF16)
    kn = (k * rk * gain_k).astype(BF16)
    vb, cb = v.astype(BF16), c.astype(BF16)
    k2, v2, q2, c2 = both(kn), both(vb), both(qn), both(cb)
    factor = HEAD_DIM**-0.5
    e = jnp.exp2(nt(qn, k2) * (factor / math.log(2.0)))
    if same is not None:
        e = jnp.where(jnp.concatenate([same, same], axis=1), e, 0.0)
    dp = nt(cb, v2)
    ps, dss = [], []
    for h in range(2):
        eh, dph = e[:, h * rows : (h + 1) * rows], dp[:, h * rows : (h + 1) * rows]
        p = eh * (1.0 / jnp.sum(eh, axis=-1, keepdims=True))
        inner = jnp.sum(p * dph, axis=-1, keepdims=True)
        dss.append((p * (dph - inner)).astype(BF16))
        ps.append(p.astype(BF16))
    o = nn(jnp.concatenate(ps, axis=1), v2)
    gv = tn(jnp.concatenate(ps, axis=0), c2)
    eq = nn(jnp.concatenate(dss, axis=1), k2)
    ek = tn(jnp.concatenate(dss, axis=0), q2)

    def norm_back(raw, inverse, gain, upstream):
        scaled = (gain * factor) * upstream
        mean0, mean1 = head_mean(raw * scaled)
        return inverse * scaled - raw * (inverse * inverse * inverse) * (mean0 * m0 + mean1 * m1)

    return o, norm_back(q, rq, gain_q, eq), norm_back(k, rk, gain_k, ek), gv


def merge(parts, width):
    columns = []
    for p in range(len(parts)):
        low = parts[p][:, :LANES]
        columns.append(low if p == 0 else low + parts[p - 1][:, LANES:])
    columns.append(parts[-1][:, LANES:])
    return jnp.concatenate(columns, axis=1)[:, :width]


def layer_norm(u):
    centre = jnp.mean(u, axis=-1, keepdims=True)
    delta = u - centre
    inverse = lax.rsqrt(jnp.mean(delta * delta, axis=-1, keepdims=True) + NORM_EPS)
    return delta * inverse, inverse


def branch_of(gm, normed, inverse, stretch):
    gn = gm * (1.0 + stretch)
    return inverse * (
        gn - jnp.mean(gn, axis=-1, keepdims=True) - normed * jnp.mean(gn * normed, axis=-1, keepdims=True)
    )


def temporal_kernel(qkv, og, u, mod, gains, w_out, w_qkv, y, sums, c_s, o_s, g_s, gm_s, ow_s):
    frames, tokens, d = og.shape
    width = w_out.shape[0]
    rows = frames * tokens
    a_s, a_g = mod[3:4, :], mod[4:5, :]

    yb = (og[...].astype(F32).reshape(rows, d) * a_g).astype(BF16)
    c_s[...] = nt(yb, w_out[...]).astype(BF16).astype(F32).reshape(frames, tokens, width)

    n = frames * GROUP
    ri = lax.broadcasted_iota(jnp.int32, (n, n), 0)
    ci = lax.broadcasted_iota(jnp.int32, (n, n), 1)
    same = (ri & (GROUP - 1)) == (ci & (GROUP - 1))

    def group(g, carry):
        at = pl.ds(pl.multiple_of(g * GROUP, GROUP), GROUP)
        outs = []
        for start, lanes, first in windows(width):
            w = pl.ds(start, lanes)
            q = qkv[0, :, at, w].astype(F32).reshape(n, lanes)
            k = qkv[1, :, at, w].astype(F32).reshape(n, lanes)
            v = qkv[2, :, at, w].astype(F32).reshape(n, lanes)
            c = c_s[:, at, w].reshape(n, lanes)
            outs.append(attention_pair(q, k, v, c, gains[2:3, w], gains[3:4, w], first, same))
        o, gq, gk, gv = [merge([t[x] for t in outs], width) for x in range(4)]
        o_s[:, at, :] = o.reshape(frames, GROUP, width)
        g_s[:, at, 0:width] = gq.reshape(frames, GROUP, width)
        g_s[:, at, width : 2 * width] = gk.reshape(frames, GROUP, width)
        g_s[:, at, 2 * width : 3 * width] = gv.reshape(frames, GROUP, width)
        return carry

    lax.fori_loop(0, tokens // GROUP, group, 0)

    ow_s[...] = nn(o_s[...].astype(BF16).reshape(rows, width), w_out[...]).reshape(frames, tokens, d)
    gm_s[...] = nt(g_s[...].astype(BF16).reshape(rows, 3 * width), w_qkv[...]).reshape(frames, tokens, d)

    def tail(f, carry):
        shift, scale, gate = carry
        y0 = og[f].astype(F32)
        normed, inverse = layer_norm(u[f].astype(F32))
        gm = gm_s[f]
        y[f] = (y0 + branch_of(gm, normed, inverse, a_s)).astype(BF16)
        return (
            shift + jnp.sum(gm, axis=0, keepdims=True),
            scale + jnp.sum(gm * normed, axis=0, keepdims=True),
            gate + jnp.sum(y0 * ow_s[f], axis=0, keepdims=True),
        )

    zero = jnp.zeros((1, d), F32)
    shift, scale, gate = lax.fori_loop(0, frames, tail, (zero, zero, zero))
    sums[0:1, :] = shift
    sums[1:2, :] = scale
    sums[2:3, :] = gate


def temporal(saved_qkv, out_grad, mid_state, modulation, gains, w_out, w_qkv):
    frames, tokens, d = out_grad.shape
    width = w_out.shape[0]
    vm = pl.BlockSpec(memory_space=pltpu.VMEM)
    flops = 2 * frames * tokens * d * width * 5
    return pl.pallas_call(
        temporal_kernel,
        out_shape=(jax.ShapeDtypeStruct(out_grad.shape, BF16), jax.ShapeDtypeStruct((3, d), F32)),
        in_specs=[vm] * 7,
        out_specs=(vm, vm),
        scratch_shapes=[
            pltpu.VMEM((frames, tokens, width), F32),
            pltpu.VMEM((frames, tokens, width), F32),
            pltpu.VMEM((frames, tokens, 3 * width), F32),
            pltpu.VMEM((frames, tokens, d), F32),
            pltpu.VMEM((frames, tokens, d), F32),
        ],
        compiler_params=pltpu.CompilerParams(vmem_limit_bytes=60 << 20),
        cost_estimate=pl.CostEstimate(flops=flops * 2, bytes_accessed=12 << 20, transcendentals=0),
        name="temporal",
    )(saved_qkv, out_grad, mid_state, modulation, gains, w_out, w_qkv)


def project_kernel(x, mod, w_qkv, q, k, v):
    src, _, tokens, d = x.shape
    width = q.shape[-1]
    normed, _ = layer_norm(x[...].astype(F32).reshape(src * tokens, d))
    m = (normed * (1.0 + mod[1:2, :]) + mod[0:1, :]).astype(BF16)
    qkv = nn(m, w_qkv[...]).astype(BF16)
    q[0] = qkv[:, :width]
    k[0] = qkv[:, width : 2 * width]
    v[0] = qkv[:, 2 * width :]


def project(x, modulation, w_qkv):
    src, frames, tokens, d = x.shape
    width = w_qkv.shape[1] // 3
    rows = src * tokens
    out = jax.ShapeDtypeStruct((frames, rows, width), BF16)
    block = pl.BlockSpec((1, rows, width), lambda f: (f, 0, 0))
    return pl.pallas_call(
        project_kernel,
        grid=(frames,),
        out_shape=(out, out, out),
        in_specs=[
            pl.BlockSpec((src, 1, tokens, d), lambda f: (0, f, 0, 0)),
            pl.BlockSpec(modulation.shape, lambda f: (0, 0)),
            pl.BlockSpec(w_qkv.shape, lambda f: (0, 0)),
        ],
        out_specs=(block, block, block),
        compiler_params=pltpu.CompilerParams(vmem_limit_bytes=60 << 20),
        cost_estimate=pl.CostEstimate(
            flops=2 * frames * rows * d * 3 * width, bytes_accessed=8 << 20, transcendentals=0
        ),
        name="project",
    )(x, modulation, w_qkv)


def spatial_kernel(x, y, q, k, v, mod, gains, w_out, w_qkv, b, sums, g_s):
    src, _, tokens, d = x.shape
    width = w_out.shape[0]
    rows = src * tokens
    a_s, a_g = mod[1:2, :], mod[2:3, :]
    yf = y[...].astype(F32).reshape(rows, d)
    c = nt((yf * a_g).astype(BF16), w_out[...]).astype(BF16).astype(F32)
    outs = []
    for start, lanes, first in windows(width):
        w = pl.ds(start, lanes)
        args = [t[0, :, w].astype(F32) for t in (q, k, v)]
        outs.append(
            attention_pair(*args, c[:, start : start + lanes], gains[0:1, w], gains[1:2, w], first, None)
        )
    o, gq, gk, gv = [merge([t[i] for t in outs], width).astype(BF16) for i in range(4)]
    g_s[:, 0:width] = gq
    g_s[:, width : 2 * width] = gk
    g_s[:, 2 * width : 3 * width] = gv
    sums[2:3, :] = jnp.sum(yf * nn(o, w_out[...]), axis=0, keepdims=True)
    gm = nt(g_s[...], w_qkv[...])
    normed, inverse = layer_norm(x[...].astype(F32).reshape(rows, d))
    sums[0:1, :] = jnp.sum(gm, axis=0, keepdims=True)
    sums[1:2, :] = jnp.sum(gm * normed, axis=0, keepdims=True)
    b[...] = branch_of(gm, normed, inverse, a_s).reshape(src, tokens, d).astype(BF16)


def spatial(f, x, y, q, k, v, modulation, gains, w_out, w_qkv):
    src, _, tokens, d = x.shape
    width = w_out.shape[0]
    rows = src * tokens
    head = pl.BlockSpec((1, rows, width), lambda i: (f, 0, 0))
    token = pl.BlockSpec((src, 1, tokens, d), lambda i: (0, f, 0, 0))

    def whole(a):
        return pl.BlockSpec(a.shape, lambda i: (0,) * a.ndim)

    flops = 2 * rows * d * width * 5 + 12 * rows * rows * width
    return pl.pallas_call(
        spatial_kernel,
        grid=(1,),
        out_shape=(jax.ShapeDtypeStruct((src, tokens, d), BF16), jax.ShapeDtypeStruct((3, d), F32)),
        in_specs=[token, token, head, head, head]
        + [whole(a) for a in (modulation, gains, w_out, w_qkv)],
        out_specs=(
            pl.BlockSpec((src, tokens, d), lambda i: (0, 0, 0)),
            pl.BlockSpec((3, d), lambda i: (0, 0)),
        ),
        scratch_shapes=[pltpu.VMEM((rows, 3 * width), BF16)],
        compiler_params=pltpu.CompilerParams(vmem_limit_bytes=60 << 20),
        cost_estimate=pl.CostEstimate(flops=flops * 2, bytes_accessed=8 << 20, transcendentals=0),
        name="spatial",
    )(x, y, q, k, v, modulation, gains, w_out, w_qkv)


def reduce_all(t, size):
    step = size // 2
    while step:
        t = t + lax.ppermute(t, "seq", [(i, i ^ step) for i in range(size)])
        step //= 2
    return t


def exchange(t):
    return lax.all_to_all(t, "seq", split_axis=0, concat_axis=0, tiled=True)


def body(size, block_input, mid_state, saved_qkv, out_grad, modulation, w_qkv_s, w_out_s, w_qkv_t, w_out_t, qk_gain):
    frames, tokens, d = out_grad.shape
    per = frames // size
    heads = w_out_t.shape[0] // HEAD_DIM
    gains = jnp.tile(qk_gain, (1, heads))
    x = exchange(block_input).reshape(size, per, tokens, d)
    y, sums_t = temporal(saved_qkv, out_grad, mid_state, modulation, gains, w_out_t, w_qkv_t)
    landed = exchange(y).reshape(size, per, tokens, d)
    q, k, v = project(x, modulation, w_qkv_s)
    results = [spatial(f, x, landed, q, k, v, modulation, gains, w_out_s, w_qkv_s) for f in range(per)]
    outgoing = jnp.stack([r[0] for r in results], axis=1).reshape(frames, tokens, d)
    returned = exchange(outgoing)
    sums_s = sum(r[1] for r in results)
    totals = reduce_all(jnp.concatenate([sums_s, sums_t], axis=0), size)
    token_count = frames * tokens * size
    input_grad = (y.astype(F32) + returned.astype(F32)).astype(BF16)
    return input_grad, totals * token_count ** (-0.5)


def solution(mesh):
    return jax.shard_map(
        functools.partial(body, mesh.shape["seq"]),
        mesh=mesh,
        in_specs=(
            P("clip", "seq", None),
            P("clip", "seq", None),
            P(None, "clip", "seq", None),
            P("clip", "seq", None),
            P("clip", None),
            P(),
            P(),
            P(),
            P(),
            P(),
        ),
        out_specs=(P("clip", "seq", None), P("clip", None)),
        check_vma=False,
    )
```
